16 devices in a mesh: tp: 4 (over z, y), dp: 4 (over x, core).
Axes of the slice: x: 2, y: 2, z: 2, core: 2. Of those that a mesh axis runs over, the one named last changes fastest.
Arguments:
- tokens: int32 [16, 1024], P('dp')
- labels: int32 [16, 1024], P('dp')
- embedding: float32 [50304, 512], P('tp')
- vec_params: float32 [16, 512], replicated
- w_qkv: float32 [2, 512, 1536], P(None, None, 'tp')
- b_qkv: float32 [2, 8, 192], P(None, 'tp')
- w_out: float32 [2, 512, 512], P(None, 'tp')
- w_up: float32 [2, 512, 2048], P(None, None, 'tp')
- b_up: float32 [2, 2048], P(None, 'tp')
- w_down: float32 [2, 2048, 512], P(None, 'tp')
- mom_embedding: float32 [50304, 512], P('tp')
- mom_vec_params: float32 [16, 512], replicated
- mom_w_qkv: float32 [2, 512, 1536], P(None, None, 'tp')
- mom_b_qkv: float32 [2, 8, 192], P(None, 'tp')
- mom_w_out: float32 [2, 512, 512], P(None, 'tp')
- mom_w_up: float32 [2, 512, 2048], P(None, None, 'tp')
- mom_b_up: float32 [2, 2048], P(None, 'tp')
- mom_w_down: float32 [2, 2048, 512], P(None, 'tp')
- vel_embedding: float32 [50304, 512], P('tp')
- vel_vec_params: float32 [16, 512], replicated
- vel_w_qkv: float32 [2, 512, 1536], P(None, None, 'tp')
- vel_b_qkv: float32 [2, 8, 192], P(None, 'tp')
- vel_w_out: float32 [2, 512, 512], P(None, 'tp')
- vel_w_up: float32 [2, 512, 2048], P(None, None, 'tp')
- vel_b_up: float32 [2, 2048], P(None, 'tp')
- vel_w_down: float32 [2, 2048, 512], P(None, 'tp')
Outputs:
- output 1: float32 [], replicated
- output 2: float32 [50304, 512], P('tp')
- output 3: float32 [16, 512], replicated
- output 4: float32 [2, 512, 1536], P(None, None, 'tp')
- output 5: float32 [2, 8, 192], P(None, 'tp')
- output 6: float32 [2, 512, 512], P(None, 'tp')
- output 7: float32 [2, 512, 2048], P(None, None, 'tp')
- output 8: float32 [2, 2048], P(None, 'tp')
- output 9: float32 [2, 2048, 512], P(None, 'tp')
- output 10: float32 [50304, 512], P('tp')
- output 11: float32 [16, 512], replicated
- output 12: float32 [2, 512, 1536], P(None, None, 'tp')
- output 13: float32 [2, 8, 192], P(None, 'tp')
- output 14: float32 [2, 512, 512], P(None, 'tp')
- output 15: float32 [2, 512, 2048], P(None, None, 'tp')
- output 16: float32 [2, 2048], P(None, 'tp')
- output 17: float32 [2, 2048, 512], P(None, 'tp')
- output 18: float32 [50304, 512], P('tp')
- output 19: float32 [16, 512], replicated
- output 20: float32 [2, 512, 1536], P(None, None, 'tp')
- output 21: float32 [2, 8, 192], P(None, 'tp')
- output 22: float32 [2, 512, 512], P(None, 'tp')
- output 23: float32 [2, 512, 2048], P(None, None, 'tp')
- output 24: float32 [2, 2048], P(None, 'tp')
- output 25: float32 [2, 2048, 512], P(None, 'tp')
- output 26: bfloat16 [50304, 512], P('tp')
- output 27: bfloat16 [16, 512], replicated
- output 28: bfloat16 [2, 512, 1536], P(None, None, 'tp')
- output 29: bfloat16 [2, 8, 192], P(None, 'tp')
- output 30: bfloat16 [2, 512, 512], P(None, 'tp')
- output 31: bfloat16 [2, 512, 2048], P(None, None, 'tp')
- output 32: bfloat16 [2, 2048], P(None, 'tp')
- output 33: bfloat16 [2, 2048, 512], P(None, 'tp')
All inputs are finite; a program needn't handle non-finite values.
Results may differ from the reference program's by a relative error of at most 0.001.
Values sent between devices are 32-bit elements.
A program may use at most 1 GiB of HBM per device.

```python
import math
import jax
import jax.numpy as jnp
from jax import lax

VOCAB = 50304
D = 512
HEADS = 8
HEAD = 64
LAYERS = 2
SEQ = 1024
BATCH = 16
STEP_COUNT = 10

FF_WIDTH = 4 * D
NUM_VECS = 4 + 6 * LAYERS
LN_EPS = 1e-5
CLIP_NORM = 1.0
BETA_ONE = 0.9
BETA_TWO = 0.95
ADAM_EPS = 1e-8
WEIGHT_DECAY = 0.1
LEARN_RATE = 1e-3
DECAYED = (True, False, True, False, True, True, False, True)
PARAM_NAMES = ('embedding', 'vec_params', 'w_qkv', 'b_qkv', 'w_out', 'w_up', 'b_up', 'w_down')


def alibi_slopes(heads):
    closest = 2 ** int(math.floor(math.log2(heads)))
    first_base = 2.0 ** (-8.0 / closest)
    slopes = [first_base ** (head_idx + 1) for head_idx in range(closest)]
    extra_base = 2.0 ** (-4.0 / closest)
    extra_count = min(closest, heads - closest)
    return slopes + [extra_base ** (2 * head_idx + 1) for head_idx in range(extra_count)]


def layer_norm(values, gain, bias):
    centred = values - jnp.mean(values, axis=-1, keepdims=True)
    variance = jnp.mean(centred * centred, axis=-1, keepdims=True)
    return centred * lax.rsqrt(variance + LN_EPS) * gain + bias


def snap_bf16(values):
    return values + lax.stop_gradient(values.astype(jnp.bfloat16).astype(jnp.float32) - values)


def adam_update(master, grad_arr, moment, velocity, decayed):
    mom_new = BETA_ONE * moment + (1.0 - BETA_ONE) * grad_arr
    vel_new = BETA_TWO * velocity + (1.0 - BETA_TWO) * grad_arr * grad_arr
    mom_hat = mom_new / (1.0 - BETA_ONE ** STEP_COUNT)
    vel_hat = vel_new / (1.0 - BETA_TWO ** STEP_COUNT)
    direction = mom_hat / (jnp.sqrt(vel_hat) + ADAM_EPS)
    if decayed:
        direction = direction + WEIGHT_DECAY * master
    return master - LEARN_RATE * direction, mom_new, vel_new


def seq_loss(params, tok_seq, lab_seq):
    embedding, vec_params, w_qkv, b_qkv, w_out, w_up, b_up, w_down = params
    positions = jnp.arange(SEQ)
    rel_pos = (positions[None, :] - positions[:, None]).astype(jnp.float32)
    causal = positions[None, :] <= positions[:, None]
    slopes = jnp.array(alibi_slopes(HEADS), dtype=jnp.float32)
    emb_snap = snap_bf16(embedding)
    resid = layer_norm(jnp.take(emb_snap, tok_seq, axis=0), vec_params[0], vec_params[1])
    for layer in range(LAYERS):
        row_base = 2 + 6 * layer
        act_in = snap_bf16(layer_norm(resid, vec_params[row_base], vec_params[row_base + 1]))
        qkv = snap_bf16(jnp.dot(act_in, snap_bf16(w_qkv[layer]), preferred_element_type=jnp.float32) + b_qkv[layer].reshape(-1))
        qkv = qkv.reshape(SEQ, HEADS, 3, HEAD)
        scores = jnp.einsum('qhd,khd->hqk', qkv[:, :, 0], qkv[:, :, 1]) * HEAD ** -0.5 + slopes[:, None, None] * rel_pos[None]
        scores = jnp.where(causal[None], scores, -jnp.inf)
        probs = snap_bf16(jax.nn.softmax(scores, axis=-1))
        context = snap_bf16(jnp.einsum('hqk,khd->qhd', probs, qkv[:, :, 2])).reshape(SEQ, D)
        resid = resid + jnp.dot(context, snap_bf16(w_out[layer]), preferred_element_type=jnp.float32) + vec_params[row_base + 2]
        mlp_in = snap_bf16(layer_norm(resid, vec_params[row_base + 3], vec_params[row_base + 4]))
        hidden = snap_bf16(jax.nn.gelu(jnp.dot(mlp_in, snap_bf16(w_up[layer]), preferred_element_type=jnp.float32) + b_up[layer], approximate=True))
        resid = resid + jnp.dot(hidden, snap_bf16(w_down[layer]), preferred_element_type=jnp.float32) + vec_params[row_base + 5]
    final_row = 2 + 6 * LAYERS
    head_in = snap_bf16(layer_norm(resid, vec_params[final_row], vec_params[final_row + 1]))
    logits = jnp.dot(head_in, emb_snap.T, preferred_element_type=jnp.float32)
    target = jnp.take_along_axis(logits, lab_seq[:, None], axis=1)[:, 0]
    return jnp.sum(jax.nn.logsumexp(logits, axis=-1) - target)


def setup_inputs(seed: int = 0) -> dict:
    keys = jax.random.split(jax.random.key(seed), 28)
    tokens = jax.random.randint(keys[0], (BATCH, SEQ), 0, VOCAB, dtype=jnp.int32)
    label_flat = jax.random.randint(keys[1], (BATCH * SEQ,), 0, VOCAB, dtype=jnp.int32)
    spread = jnp.arange(8, dtype=jnp.int32) * (VOCAB // 8) + jax.random.randint(keys[2], (8,), 0, VOCAB // 8, dtype=jnp.int32)
    labels = label_flat.at[:8].set(spread).reshape(BATCH, SEQ)
    row_base = jnp.array([1.0, 0.0] + [1.0, 0.0, 0.0, 1.0, 0.0, 0.0] * LAYERS + [16.0, 0.0], dtype=jnp.float32)
    row_scale = jnp.array([0.2] * (2 + 6 * LAYERS) + [3.2, 0.5], dtype=jnp.float32)
    shapes = [(VOCAB, D), (NUM_VECS, D), (LAYERS, D, 3 * D), (LAYERS, HEADS, 3 * HEAD), (LAYERS, D, D), (LAYERS, D, FF_WIDTH), (LAYERS, FF_WIDTH), (LAYERS, FF_WIDTH, D)]
    scales = [0.2 * D ** -0.5, 1.0, D ** -0.5, 0.2, D ** -0.5, D ** -0.5, 0.2, FF_WIDTH ** -0.5]
    masters = [jax.random.normal(keys[3 + slot], shapes[slot], jnp.float32) * scales[slot] for slot in range(8)]
    masters[1] = row_base[:, None] + row_scale[:, None] * masters[1]
    grad_scale = float(VOCAB * D + NUM_VECS * D + LAYERS * (12 * D * D + 3 * D + FF_WIDTH)) ** -0.5
    moms = [jax.random.normal(keys[11 + slot], shapes[slot], jnp.float32) * grad_scale for slot in range(8)]
    vels = [jax.random.uniform(keys[19 + slot], shapes[slot], jnp.float32, 0.25, 2.0) * grad_scale ** 2 for slot in range(8)]
    result = {'tokens': tokens, 'labels': labels}
    for slot in range(8):
        result[PARAM_NAMES[slot]] = masters[slot]
    for slot in range(8):
        result['mom_' + PARAM_NAMES[slot]] = moms[slot]
    for slot in range(8):
        result['vel_' + PARAM_NAMES[slot]] = vels[slot]
    return result


def reference(tokens, labels, embedding, vec_params, w_qkv, b_qkv, w_out, w_up, b_up, w_down, mom_embedding, mom_vec_params, mom_w_qkv, mom_b_qkv, mom_w_out, mom_w_up, mom_b_up, mom_w_down, vel_embedding, vel_vec_params, vel_w_qkv, vel_b_qkv, vel_w_out, vel_w_up, vel_b_up, vel_w_down):
    masters = (embedding, vec_params, w_qkv, b_qkv, w_out, w_up, b_up, w_down)
    moms = (mom_embedding, mom_vec_params, mom_w_qkv, mom_b_qkv, mom_w_out, mom_w_up, mom_b_up, mom_w_down)
    vels = (vel_embedding, vel_vec_params, vel_w_qkv, vel_b_qkv, vel_w_out, vel_w_up, vel_b_up, vel_w_down)

    def total_loss(params):
        def one_seq(pair):
            return seq_loss(params, pair[0], pair[1])
        per_seq = lax.map(jax.checkpoint(one_seq), (tokens, labels))
        return jnp.sum(per_seq) / (BATCH * SEQ)

    loss, grads = jax.value_and_grad(total_loss)(masters)
    sq_total = sum(jnp.sum(grad_arr * grad_arr) for grad_arr in grads)
    clip_coef = jnp.minimum(1.0, CLIP_NORM / (jnp.sqrt(sq_total) + 1e-6))
    updated = [adam_update(masters[slot], grads[slot] * clip_coef, moms[slot], vels[slot], DECAYED[slot]) for slot in range(8)]
    new_masters = [entry[0] for entry in updated]
    new_moms = [entry[1] for entry in updated]
    new_vels = [entry[2] for entry in updated]
    new_bf16 = [entry.astype(jnp.bfloat16) for entry in new_masters]
    return (loss, *new_masters, *new_moms, *new_vels, *new_bf16)
```

```python
import functools
import math
import jax
import jax.numpy as jnp
from jax import lax
from jax.experimental import pallas as pl
from jax.experimental.pallas import tpu as pltpu
from jax.sharding import PartitionSpec as P

LN_EPS = 1e-5
CLIP_NORM = 1.0
BETA_ONE = 0.9
BETA_TWO = 0.95
ADAM_EPS = 1e-8
WEIGHT_DECAY = 0.1
LEARN_RATE = 1e-3
STEP_COUNT = 10
DECAYED = (True, False, True, False, True, True, False, True)
PARAM_SPECS = (P('tp', None), P(None, None), P(None, None, 'tp'), P(None, 'tp', None), P(None, 'tp', None), P(None, None, 'tp'), P(None, 'tp'), P(None, 'tp', None))
ALL = ('tp', 'dp')
F32 = jnp.float32
BF16 = jnp.bfloat16
NN = (((1,), (0,)), ((), ()))
NT = (((1,), (1,)), ((), ()))
TN = (((0,), (0,)), ((), ()))
CHUNKS = 4
HEAD_TOK = 512
VOC_BLK = 256
Q_BLK = 256
PAD_ROWS = 8
VMEM_CAP = 60 * 1024 * 1024


def alibi_slopes(heads):
    closest = 2 ** int(math.floor(math.log2(heads)))
    first_base = 2.0 ** (-8.0 / closest)
    slopes = [first_base ** (head_idx + 1) for head_idx in range(closest)]
    extra_base = 2.0 ** (-4.0 / closest)
    extra_count = min(closest, heads - closest)
    return slopes + [extra_base ** (2 * head_idx + 1) for head_idx in range(extra_count)]


def layer_norm(values, gain, bias):
    centred = values - jnp.mean(values, axis=-1, keepdims=True)
    variance = jnp.mean(centred * centred, axis=-1, keepdims=True)
    return centred * lax.rsqrt(variance + LN_EPS) * gain + bias


def gelu_tanh(values):
    return jax.nn.gelu(values, approximate=True)


def adam_update(master, grad_arr, moment, velocity, decayed):
    mom_new = BETA_ONE * moment + (1.0 - BETA_ONE) * grad_arr
    vel_new = BETA_TWO * velocity + (1.0 - BETA_TWO) * grad_arr * grad_arr
    mom_hat = mom_new / (1.0 - BETA_ONE ** STEP_COUNT)
    vel_hat = vel_new / (1.0 - BETA_TWO ** STEP_COUNT)
    direction = mom_hat / (jnp.sqrt(vel_hat) + ADAM_EPS)
    if decayed:
        direction = direction + WEIGHT_DECAY * master
    return master - LEARN_RATE * direction, mom_new, vel_new


def mm(lhs, rhs, dims=NN):
    return lax.dot_general(lhs, rhs, dims, preferred_element_type=F32)


def stats_kernel(voc, lab_ref, x_ref, e_ref, m_ref, s_ref, t_ref):
    xb = x_ref[...].astype(BF16)
    lab = lab_ref[...]
    tok = xb.shape[0]
    full = voc // VOC_BLK

    def block(start, rows, carry):
        run_max, run_sum, run_tgt = carry
        logits = mm(e_ref[pl.ds(start, rows), :], xb, NT)
        row = lax.broadcasted_iota(jnp.int32, (rows, tok), 0) + start
        run_tgt = run_tgt + jnp.sum(jnp.where(row == lab, logits, 0.0), axis=0, keepdims=True)
        if rows != VOC_BLK:
            logits = jnp.where(row < voc, logits, -jnp.inf)
        new_max = jnp.maximum(run_max, jnp.max(logits, axis=0, keepdims=True))
        run_sum = run_sum * jnp.exp(run_max - new_max) + jnp.sum(jnp.exp(logits - new_max), axis=0, keepdims=True)
        return new_max, run_sum, run_tgt

    carry = (jnp.full((1, tok), -jnp.inf, F32), jnp.zeros((1, tok), F32), jnp.zeros((1, tok), F32))
    carry = lax.fori_loop(0, full, lambda idx, c: block(pl.multiple_of(idx * VOC_BLK, VOC_BLK), VOC_BLK, c), carry)
    tail = e_ref.shape[0] - full * VOC_BLK
    if tail:
        carry = block(full * VOC_BLK, tail, carry)
    m_ref[...], s_ref[...], t_ref[...] = carry


def head_stats(lab, x_all, e_pad, voc):
    tok, width = x_all.shape
    vec = pl.BlockSpec((1, HEAD_TOK), lambda i: (0, i))
    out = jax.ShapeDtypeStruct((1, tok), F32)
    return pl.pallas_call(
        functools.partial(stats_kernel, voc),
        grid=(tok // HEAD_TOK,),
        in_specs=[vec, pl.BlockSpec((HEAD_TOK, width), lambda i: (i, 0)), pl.BlockSpec(e_pad.shape, lambda i: (0, 0))],
        out_specs=[vec, vec, vec],
        out_shape=[out, out, out],
        compiler_params=pltpu.CompilerParams(vmem_limit_bytes=VMEM_CAP),
        cost_estimate=pl.CostEstimate(flops=2 * tok * voc * width, bytes_accessed=tok * width * 4 + voc * width * 2, transcendentals=tok * voc),
        name='head_stats',
    )(lab, x_all, e_pad)


def hgrad_kernel(voc, inv_n, first, *refs):
    if first:
        lab_ref, lse_ref, x_ref, e_ref, et_ref, g_ref, dh_ref, acc_ref = refs
    else:
        lab_ref, lse_ref, x_ref, e_ref, et_ref, gin_ref, g_ref, dh_ref, acc_ref = refs
    xb = x_ref[...].astype(BF16)
    lab = lab_ref[...]
    lse = lse_ref[...]
    tok = xb.shape[0]
    full = voc // VOC_BLK

    @pl.when(pl.program_id(0) == 0)
    def _():
        if first:
            g_ref[...] = jnp.zeros_like(g_ref)
        else:
            g_ref[...] = gin_ref[...]

    acc_ref[...] = jnp.zeros_like(acc_ref)

    def block(start, rows, keep):
        logits = mm(e_ref[pl.ds(start, rows), :], xb, NT)
        row = lax.broadcasted_iota(jnp.int32, (rows, tok), 0) + start
        prob = jnp.exp(logits - lse)
        grad = jnp.where(row == lab, prob - 1.0, prob) * inv_n
        if rows != VOC_BLK:
            grad = jnp.where(row < voc, grad, 0.0)
        grad = grad.astype(BF16)
        gemb = mm(grad, xb)
        g_ref[pl.ds(start, keep), :] += gemb[:keep]
        acc_ref[...] += mm(et_ref[:, pl.ds(start, rows)], grad)

    def body(idx, carry):
        block(pl.multiple_of(idx * VOC_BLK, VOC_BLK), VOC_BLK, VOC_BLK)
        return carry

    lax.fori_loop(0, full, body, 0)
    tail = e_ref.shape[0] - full * VOC_BLK
    if tail:
        block(full * VOC_BLK, tail, voc - full * VOC_BLK)
    dh_ref[...] = acc_ref[...].T


def head_grads(lab, lse, x_all, e_pad, e_tr, g_in, voc, inv_n):
    tok, width = x_all.shape
    first = g_in is None
    vec = pl.BlockSpec((1, HEAD_TOK), lambda i: (0, i))
    rows = pl.BlockSpec((HEAD_TOK, width), lambda i: (i, 0))
    whole = pl.BlockSpec((voc, width), lambda i: (0, 0))
    in_specs = [vec, vec, rows, pl.BlockSpec(e_pad.shape, lambda i: (0, 0)), pl.BlockSpec(e_tr.shape, lambda i: (0, 0))]
    args = [lab, lse, x_all, e_pad, e_tr]
    if not first:
        in_specs.append(whole)
        args.append(g_in)
    return pl.pallas_call(
        functools.partial(hgrad_kernel, voc, inv_n, first),
        grid=(tok // HEAD_TOK,),
        in_specs=in_specs,
        out_specs=[whole, rows],
        out_shape=[jax.ShapeDtypeStruct((voc, width), F32), jax.ShapeDtypeStruct((tok, width), F32)],
        scratch_shapes=[pltpu.VMEM((width, HEAD_TOK), F32)],
        input_output_aliases={} if first else {5: 0},
        compiler_params=pltpu.CompilerParams(vmem_limit_bytes=VMEM_CAP),
        cost_estimate=pl.CostEstimate(flops=6 * tok * voc * width, bytes_accessed=tok * width * 8 + voc * width * 12, transcendentals=tok * voc),
        name='head_grads',
    )(*args)


def probs_tr(query, key_blk, slope, scale, q_start):
    keys = key_blk.shape[0]
    rows = query.shape[0]
    key_pos = lax.broadcasted_iota(jnp.int32, (keys, rows), 0)
    qry_pos = lax.broadcasted_iota(jnp.int32, (keys, rows), 1) + q_start
    rel = key_pos - qry_pos
    scores = mm(key_blk, query, NT) * scale + slope * rel.astype(F32)
    scores = jnp.where(rel <= 0, scores, -jnp.inf)
    shifted = jnp.exp(scores - jnp.max(scores, axis=0, keepdims=True))
    return shifted / jnp.sum(shifted, axis=0, keepdims=True)


def attn_fwd_kernel(scale, head_dim, slope_ref, qkv_ref, ctx_ref):
    seq = qkv_ref.shape[0]
    for sub in range(2):
        slope = slope_ref[pl.program_id(0) * 2 + sub]
        base = sub * 3 * head_dim
        value_tr = qkv_ref[:, base + 2 * head_dim:base + 3 * head_dim].T
        for q_start in range(0, seq, Q_BLK):
            keys = q_start + Q_BLK
            query = qkv_ref[q_start:keys, base:base + head_dim]
            key_blk = qkv_ref[0:keys, base + head_dim:base + 2 * head_dim]
            probs = probs_tr(query, key_blk, slope, scale, q_start)
            ctx_tr = mm(value_tr[:, 0:keys], probs.astype(BF16))
            ctx_ref[q_start:keys, sub * head_dim:(sub + 1) * head_dim] = ctx_tr.T.astype(BF16)


def attn_bwd_kernel(scale, head_dim, slope_ref, qkv_ref, dctx_ref, out_ref):
    seq = qkv_ref.shape[0]
    out_ref[...] = jnp.zeros_like(out_ref)
    for sub in range(2):
        slope = slope_ref[pl.program_id(0) * 2 + sub]
        base = sub * 3 * head_dim
        q_cols = slice(base, base + head_dim)
        k_cols = slice(base + head_dim, base + 2 * head_dim)
        v_cols = slice(base + 2 * head_dim, base + 3 * head_dim)
        key_tr = qkv_ref[:, k_cols].T
        for q_start in range(0, seq, Q_BLK):
            keys = q_start + Q_BLK
            query = qkv_ref[q_start:keys, q_cols]
            key_blk = qkv_ref[0:keys, k_cols]
            value_blk = qkv_ref[0:keys, v_cols]
            dctx = dctx_ref[q_start:keys, sub * head_dim:(sub + 1) * head_dim]
            probs = probs_tr(query, key_blk, slope, scale, q_start)
            d_probs = mm(value_blk, dctx, NT)
            inner = jnp.sum(probs * d_probs, axis=0, keepdims=True)
            d_scores = (probs * (d_probs - inner) * scale).astype(BF16)
            out_ref[0:keys, v_cols] += mm(probs.astype(BF16), dctx)
            out_ref[0:keys, k_cols] += mm(d_scores, query)
            out_ref[q_start:keys, q_cols] = mm(key_tr[:, 0:keys], d_scores).T


def attn_forward(qkv, slopes, heads, head_dim):
    seq = qkv.shape[0]
    return pl.pallas_call(
        functools.partial(attn_fwd_kernel, head_dim ** -0.5, head_dim),
        grid=(heads // 2,),
        in_specs=[pl.BlockSpec(memory_space=pltpu.SMEM), pl.BlockSpec((seq, 6 * head_dim), lambda i: (0, i))],
        out_specs=pl.BlockSpec((seq, 2 * head_dim), lambda i: (0, i)),
        out_shape=jax.ShapeDtypeStruct((seq, heads * head_dim), BF16),
        compiler_params=pltpu.CompilerParams(vmem_limit_bytes=VMEM_CAP),
        cost_estimate=pl.CostEstimate(flops=16 * heads * seq * seq * head_dim, bytes_accessed=seq * heads * head_dim * 8, transcendentals=heads * seq * seq),
        name='attn_fwd',
    )(slopes, qkv)


def attn_backward(qkv, dctx, slopes, heads, head_dim):
    seq = qkv.shape[0]
    return pl.pallas_call(
        functools.partial(attn_bwd_kernel, head_dim ** -0.5, head_dim),
        grid=(heads // 2,),
        in_specs=[pl.BlockSpec(memory_space=pltpu.SMEM), pl.BlockSpec((seq, 6 * head_dim), lambda i: (0, i)), pl.BlockSpec((seq, 2 * head_dim), lambda i: (0, i))],
        out_specs=pl.BlockSpec((seq, 6 * head_dim), lambda i: (0, i)),
        out_shape=jax.ShapeDtypeStruct((seq, 3 * heads * head_dim), F32),
        compiler_params=pltpu.CompilerParams(vmem_limit_bytes=VMEM_CAP),
        cost_estimate=pl.CostEstimate(flops=40 * heads * seq * seq * head_dim, bytes_accessed=seq * heads * head_dim * 20, transcendentals=heads * seq * seq),
        name='attn_bwd',
    )(slopes, qkv, dctx)


def lookup_kernel(blk_rows, ids_ref, perm_ref, bound_ref, d_hbm, g_ref, out_ref, sq_ref, d_ref, sem):
    blk = pl.program_id(0)

    @pl.when(blk == 0)
    def _():
        copy = pltpu.make_async_copy(d_hbm, d_ref, sem)
        copy.start()
        copy.wait()
        sq_ref[...] = jnp.zeros_like(sq_ref)

    out_ref[...] = g_ref[...]
    first = bound_ref[blk]
    last = bound_ref[blk + 1]
    base = bound_ref[bound_ref.shape[0] - 1] + blk * blk_rows

    def body(idx, carry):
        row = ids_ref[idx] - base
        out_ref[pl.ds(row, 1), :] += d_ref[pl.ds(perm_ref[idx], 1), :]
        return carry

    lax.fori_loop(first, last, body, 0)
    vals = out_ref[...]
    sq_ref[...] += jnp.sum((vals * vals).reshape(blk_rows // 8, 8, vals.shape[1]), axis=0)


def lookup_add(ids, perm, bounds, d_all, g_head, blk_rows):
    rows, width = g_head.shape
    spec = pl.BlockSpec((blk_rows, width), lambda i, *_: (i, 0))
    return pl.pallas_call(
        functools.partial(lookup_kernel, blk_rows),
        grid_spec=pltpu.PrefetchScalarGridSpec(
            num_scalar_prefetch=3,
            grid=(rows // blk_rows,),
            in_specs=[pl.BlockSpec(memory_space=pl.ANY), spec],
            out_specs=[spec, pl.BlockSpec((8, width), lambda i, *_: (0, 0))],
            scratch_shapes=[pltpu.VMEM(d_all.shape, F32), pltpu.SemaphoreType.DMA],
        ),
        out_shape=[jax.ShapeDtypeStruct((rows, width), F32), jax.ShapeDtypeStruct((8, width), F32)],
        compiler_params=pltpu.CompilerParams(vmem_limit_bytes=VMEM_CAP),
        cost_estimate=pl.CostEstimate(flops=rows * width * 40, bytes_accessed=rows * width * 8 + d_all.shape[0] * width * 4, transcendentals=0),
        name='lookup_add',
    )(ids, perm, bounds, d_all, g_head)


def pick(values, start, size, axis):
    return lax.dynamic_slice_in_dim(values, start, size, axis)


def solution(mesh):
    tp_size = mesh.shape['tp']
    dp_size = mesh.shape['dp']
    n_dev = tp_size * dp_size

    def device_step(tokens, labels, *state):
        masters = state[0:8]
        moms = state[8:16]
        vels = state[16:24]
        embedding, vec_params, w_qkv, b_qkv, w_out, w_up, b_up, w_down = masters
        tp_rank = lax.axis_index('tp')
        dp_rank = lax.axis_index('dp')
        vocab_loc, width = embedding.shape
        voc = vocab_loc // dp_size
        seq_len = tokens.shape[1]
        n_total = seq_len * tokens.shape[0] * dp_size
        layers = w_qkv.shape[0]
        head_dim = b_qkv.shape[2] // 3
        heads = b_qkv.shape[1] * tp_size
        qkv_q = w_qkv.shape[2] // dp_size
        out_q = w_out.shape[1] // dp_size
        ff_q = w_up.shape[2] // dp_size
        slopes = jnp.array(alibi_slopes(heads), dtype=F32)

        own = jnp.concatenate([pick(tokens, tp_rank, 1, 0), pick(labels, tp_rank, 1, 0)], axis=0)
        both = lax.all_gather(own, ALL)
        tok_all = both[:, 0]
        lab_all = both[:, 1]

        id_local = tokens.reshape(-1) - tp_rank * vocab_loc
        in_shard = (id_local >= 0) & (id_local < vocab_loc)
        picked = jnp.take(embedding, jnp.clip(id_local, 0, vocab_loc - 1), axis=0)
        picked = jnp.where(in_shard[:, None], lax.reduce_precision(picked, 8, 7), 0.0)
        x_embed = lax.psum_scatter(picked, 'tp', scatter_dimension=0, tiled=True)

        weights = []
        for layer in range(layers):
            bias_q = pick(b_qkv[layer].reshape(-1), dp_rank * qkv_q, qkv_q, 0)
            bias_u = pick(b_up[layer], dp_rank * ff_q, ff_q, 0)
            bias_row = jnp.concatenate([bias_q, bias_u, jnp.zeros((width - qkv_q - ff_q,), F32)])[None]
            pack = jnp.concatenate([
                pick(w_qkv[layer], dp_rank * qkv_q, qkv_q, 1).T,
                pick(w_out[layer], dp_rank * out_q, out_q, 0),
                pick(w_up[layer], dp_rank * ff_q, ff_q, 1).T,
                pick(w_down[layer], dp_rank * ff_q, ff_q, 0),
                jnp.pad(bias_row, ((0, PAD_ROWS - 1), (0, 0)))], axis=0)
            got = lax.optimization_barrier(lax.all_gather(pack, ALL))
            at = 0
            parts = []
            for rows in (qkv_q, out_q, ff_q, ff_q):
                parts.append(got[:, at:at + rows].reshape(n_dev * rows, width).astype(BF16))
                at += rows
            bias = got[:, at]
            weights.append(tuple(parts) + (bias[:, :qkv_q].reshape(-1), bias[:, qkv_q:qkv_q + ff_q].reshape(-1)))

        emb_slice = pick(embedding, dp_rank * voc, voc, 0).astype(BF16)
        voc_pad = -(-voc // 16) * 16
        e_pad = jnp.pad(emb_slice, ((0, voc_pad - voc), (0, 0)))
        e_tr = jnp.pad(emb_slice, ((0, -(-voc // 128) * 128 - voc), (0, 0))).T

        resid, ln_zero_vjp = jax.vjp(layer_norm, x_embed, vec_params[0], vec_params[1])
        saved = []
        for layer in range(layers):
            wqkv_t, wout_b, wup_t, wdown_b, bias_q, bias_u = weights[layer]
            row_base = 2 + 6 * layer
            normed_one, ln_one_vjp = jax.vjp(layer_norm, resid, vec_params[row_base], vec_params[row_base + 1])
            act_in = normed_one.astype(BF16)
            qkv = (mm(act_in, wqkv_t, NT) + bias_q).astype(BF16)
            context = attn_forward(qkv, slopes, heads, head_dim)
            mid = resid + mm(context, wout_b) + vec_params[row_base + 2]
            normed_two, ln_two_vjp = jax.vjp(layer_norm, mid, vec_params[row_base + 3], vec_params[row_base + 4])
            mlp_in = normed_two.astype(BF16)
            pre_act = mm(mlp_in, wup_t, NT) + bias_u
            act_out, gelu_vjp = jax.vjp(gelu_tanh, pre_act)
            hidden = act_out.astype(BF16)
            resid = mid + mm(hidden, wdown_b) + vec_params[row_base + 5]
            saved.append((ln_one_vjp, act_in, qkv, context, ln_two_vjp, mlp_in, gelu_vjp, hidden))

        final_row = 2 + 6 * layers
        normed_fin, ln_fin_vjp = jax.vjp(layer_norm, resid, vec_params[final_row], vec_params[final_row + 1])

        step = seq_len // CHUNKS
        lab_loc = lab_all - (tp_rank * vocab_loc + dp_rank * voc)
        x_parts = []
        lab_parts = []
        stats = []
        for part in range(CHUNKS):
            x_all = lax.all_gather(normed_fin[part * step:(part + 1) * step], ALL).reshape(n_dev * step, width)
            lab = lab_loc[:, part * step:(part + 1) * step].reshape(1, -1)
            x_parts.append(x_all)
            lab_parts.append(lab)
            stats.append(jnp.concatenate(head_stats(lab, x_all, e_pad, voc), axis=0))
        lses = []
        loss_sum = 0.0
        for pair in range(0, CHUNKS, 2):
            got = lax.all_gather(jnp.concatenate(stats[pair:pair + 2], axis=1), ALL)
            glob_max = jnp.max(got[:, 0], axis=0)
            lse = glob_max + jnp.log(jnp.sum(got[:, 1] * jnp.exp(got[:, 0] - glob_max), axis=0))
            loss_sum = loss_sum + jnp.sum(lse - jnp.sum(got[:, 2], axis=0))
            half = lse.shape[0] // 2
            lses += [lse[None, :half], lse[None, half:]]
        loss = loss_sum / n_total

        g_slice = None
        d_parts = []
        for part in range(CHUNKS):
            g_slice, d_part = head_grads(lab_parts[part], lses[part], x_parts[part], e_pad, e_tr, g_slice, voc, 1.0 / n_total)
            d_parts.append(lax.psum_scatter(d_part.reshape(n_dev, step, width), ALL, scatter_dimension=0, tiled=False))
        d_head = jnp.concatenate(d_parts, axis=0)
        g_head = lax.all_gather(g_slice, 'dp').reshape(vocab_loc, width)

        vec_grads = {}
        d_resid, vec_grads[final_row], vec_grads[final_row + 1] = ln_fin_vjp(d_head)
        summed = {}
        for layer in reversed(range(layers)):
            ln_one_vjp, act_in, qkv, context, ln_two_vjp, mlp_in, gelu_vjp, hidden = saved[layer]
            wqkv_t, wout_b, wup_t, wdown_b, _, _ = weights[layer]
            row_base = 2 + 6 * layer
            vec_grads[row_base + 5] = jnp.sum(d_resid, axis=0)
            d_out = d_resid.astype(BF16)
            g_down = mm(hidden, d_out, TN)
            d_pre = gelu_vjp(mm(d_out, wdown_b, NT))[0]
            g_bup = jnp.sum(d_pre, axis=0)
            d_pre_b = d_pre.astype(BF16)
            g_up = mm(d_pre_b, mlp_in, TN)
            d_mid_ln, vec_grads[row_base + 3], vec_grads[row_base + 4] = ln_two_vjp(mm(d_pre_b, wup_t))
            d_mid = d_resid + d_mid_ln
            vec_grads[row_base + 2] = jnp.sum(d_mid, axis=0)
            d_attn = d_mid.astype(BF16)
            g_out = mm(context, d_attn, TN)
            d_context = mm(d_attn, wout_b, NT).astype(BF16)
            d_qkv = attn_backward(qkv, d_context, slopes, heads, head_dim)
            g_bqkv = jnp.sum(d_qkv, axis=0)
            d_qkv_b = d_qkv.astype(BF16)
            g_qkv = mm(d_qkv_b, act_in, TN)
            d_res_ln, vec_grads[row_base], vec_grads[row_base + 1] = ln_one_vjp(mm(d_qkv_b, wqkv_t))
            d_resid = d_mid + d_res_ln
            bias_rows = jnp.concatenate([g_bqkv.reshape(n_dev, qkv_q), g_bup.reshape(n_dev, ff_q), jnp.zeros((n_dev, width - qkv_q - ff_q), F32)], axis=1)
            summed[layer] = jnp.concatenate([
                g_qkv.reshape(n_dev, qkv_q, width), g_out.reshape(n_dev, out_q, width),
                g_up.reshape(n_dev, ff_q, width), g_down.reshape(n_dev, ff_q, width),
                jnp.pad(bias_rows[:, None], ((0, 0), (0, PAD_ROWS - 1), (0, 0)))], axis=1)
            if layer > 0:
                summed[layer] = lax.psum_scatter(summed[layer], ALL, scatter_dimension=0, tiled=False)
        d_embed, vec_grads[0], vec_grads[1] = ln_zero_vjp(d_resid)
        d_all = lax.all_gather(d_embed, ALL).reshape(n_total, width)
        summed[0] = lax.psum_scatter(summed[0], ALL, scatter_dimension=0, tiled=False)
        vec_grad = lax.psum(jnp.stack([vec_grads[row] for row in range(final_row + 2)]), ALL)

        blk_rows = vocab_loc // 12
        ids, perm = lax.sort((tok_all.reshape(-1), lax.iota(jnp.int32, n_total)), num_keys=1)
        edges = tp_rank * vocab_loc + jnp.arange(13, dtype=jnp.int32) * blk_rows
        bounds = jnp.sum((tok_all.reshape(-1)[None] < edges[:, None]).astype(jnp.int32), axis=1)
        bounds = jnp.concatenate([bounds, edges[:1]])
        g_emb, sq_emb = lookup_add(ids, perm, bounds, d_all, g_head, blk_rows)

        sq_dev = jnp.sum(sq_emb) / dp_size + sum(jnp.sum(summed[layer] * summed[layer]) for layer in range(layers))
        sq_total = lax.psum(sq_dev, ALL) + jnp.sum(vec_grad * vec_grad)
        clip_coef = jnp.minimum(1.0, CLIP_NORM / (jnp.sqrt(sq_total) + 1e-6))

        per_layer = []
        for layer in range(layers):
            got = lax.all_gather(summed[layer], 'dp')
            at = 0
            parts = []
            for rows in (qkv_q, out_q, ff_q, ff_q):
                parts.append(got[:, at:at + rows].reshape(dp_size * rows, width))
                at += rows
            bias = got[:, at]
            per_layer.append((parts[0].T, bias[:, :qkv_q].reshape(b_qkv.shape[1:]), parts[1], parts[2].T, bias[:, qkv_q:qkv_q + ff_q].reshape(-1), parts[3]))
        grads = [g_emb, vec_grad] + [jnp.stack([per_layer[layer][slot] for layer in range(layers)]) for slot in range(6)]
        updated = [adam_update(masters[slot], grads[slot] * clip_coef, moms[slot], vels[slot], DECAYED[slot]) for slot in range(8)]
        new_masters = [entry[0] for entry in updated]
        new_moms = [entry[1] for entry in updated]
        new_vels = [entry[2] for entry in updated]
        new_bf16 = [entry.astype(BF16) for entry in new_masters]
        return (loss, *new_masters, *new_moms, *new_vels, *new_bf16)

    data_spec = P('dp', None)
    return jax.shard_map(device_step, mesh=mesh, in_specs=(data_spec, data_spec) + PARAM_SPECS * 3, out_specs=(P(),) + PARAM_SPECS * 4, check_vma=False)
```
